32 devices in a mesh: depth: 4 (over y, x), area: 8 (over z, core).
Axes of the slice: x: 2, y: 2, z: 4, core: 2. Of those that a mesh axis runs over, the one named last changes fastest.
Arguments:
- states: float32 [8, 64, 128, 768], P(None, 'depth', 'area'), may hold values from 0 to 1
- tissue: int32 [16, 32, 192], P('depth', 'area'), may hold values 0 or 1
- fiber: int32 [16, 32, 192], P('depth', 'area'), may hold values from 0 to 7
Outputs:
- final_states: float32 [8, 64, 128, 768], P(None, 'depth', 'area')
- images: float32 [2, 2, 4, 128, 768], P(None, None, None, 'area', 'depth')
The draws below stay inside these ranges and needn't reach their ends.
All inputs are finite; a program needn't handle non-finite values. No bound on the sum of `tissue` on one device may be relied on, other than what follows from the above.
Results may differ from the reference program's by a relative error of at most 0.0002.
Values sent between devices are 32-bit elements; how exact they have to be, the bound alone decides.
A program may use at most 128 MiB of HBM per device.

```python
import math
import jax
import jax.numpy as jnp

NZ = 768
STATES = 8
BLK = 4
CLASSES = 8
STEPS = 2
NX = 64
NY = 128


def plant(drawn, key, smallest, largest):
    shape = drawn.shape
    place = [jax.random.randint(jax.random.fold_in(key, axis), (), 0, shape[axis]) for axis in range(len(shape))]
    drawn = drawn.at[tuple(place)].set(smallest)
    longest = shape.index(max(shape))
    place[longest] = (place[longest] + 1) % shape[longest]
    return drawn.at[tuple(place)].set(largest)


def level_of(stream_key, extent, shards, least, largest):
    def one(dim, shards_of):
        draws = jax.random.uniform(jax.random.fold_in(jax.random.fold_in(stream_key, 6), dim), (shards_of,), jnp.float32, least / len(shards), largest / len(shards))
        return jnp.repeat(jnp.exp(draws), extent[dim] // shards_of).reshape((-1,) + (1,) * (len(extent) - dim - 1))

    factor_of = one(*shards[0])
    for cut in shards[1:]:
        factor_of = factor_of * one(*cut)
    return factor_of


def setup_inputs(seed: int = 0) -> dict:
    streams_of = jax.random.split(jax.random.key(seed), 4)
    return {
        "states": jnp.clip(1.0 * jax.random.uniform(streams_of[0], (STATES, NX, NY, NZ), jnp.float32) ** level_of(streams_of[0], (STATES, NX, NY, NZ), ((1, 4), (2, 8)), -0.2, 0.2), 0.0, 1.0),
        "tissue": plant((jax.random.randint(streams_of[1], (NX // BLK, NY // BLK, NZ // BLK), 0, 4) < 3).astype(jnp.int32), jax.random.fold_in(streams_of[1], 1), 0, 1),
        "fiber": plant(jax.random.randint(streams_of[2], (NX // BLK, NY // BLK, NZ // BLK), 0, CLASSES), jax.random.fold_in(streams_of[2], 1), 0, CLASSES - 1).astype(jnp.int32),
    }


TIME_STEP = 0.15
SIGMA_LONG = 1.0
SIGMA_CROSS = 0.3
SLOPES = (8.0, -8.0, 6.0, 5.0, -5.0, -3.0)
MIDDLES = (0.2, 0.4, 0.3, 0.5, 0.6, 0.5)
RATES = (3.0, 0.5, 1.0, 0.8, 0.3, 0.1)
OPACITY = (0.012, 0.010)


def expand(blocks):
    first, second, third = blocks.shape
    wide = jnp.broadcast_to(blocks[:, None, :, None, :, None], (first, BLK, second, BLK, third, BLK))
    return wide.reshape(first * BLK, second * BLK, third * BLK)


def tensor(fiber):
    kind = fiber.astype(jnp.float32)
    polar = math.pi * (kind + 0.5) / CLASSES
    azimuth = 2.3 * kind
    along_x = jnp.cos(polar)
    along_y = jnp.sin(polar) * jnp.cos(azimuth)
    along_z = jnp.sin(polar) * jnp.sin(azimuth)
    spread = SIGMA_LONG - SIGMA_CROSS
    parts = (SIGMA_CROSS + spread * along_x * along_x, SIGMA_CROSS + spread * along_y * along_y,
             SIGMA_CROSS + spread * along_z * along_z, spread * along_x * along_y,
             spread * along_x * along_z, spread * along_y * along_z)
    return tuple(expand(item) for item in parts)


def diffuse(padded, comps):
    centre = padded[1:-1, 1:-1, 1:-1]
    second_x = padded[2:, 1:-1, 1:-1] - 2.0 * centre + padded[:-2, 1:-1, 1:-1]
    second_y = padded[1:-1, 2:, 1:-1] - 2.0 * centre + padded[1:-1, :-2, 1:-1]
    second_z = padded[1:-1, 1:-1, 2:] - 2.0 * centre + padded[1:-1, 1:-1, :-2]
    cross_xy = 0.25 * (padded[2:, 2:, 1:-1] - padded[2:, :-2, 1:-1] - padded[:-2, 2:, 1:-1] + padded[:-2, :-2, 1:-1])
    cross_xz = 0.25 * (padded[2:, 1:-1, 2:] - padded[2:, 1:-1, :-2] - padded[:-2, 1:-1, 2:] + padded[:-2, 1:-1, :-2])
    cross_yz = 0.25 * (padded[1:-1, 2:, 2:] - padded[1:-1, 2:, :-2] - padded[1:-1, :-2, 2:] + padded[1:-1, :-2, :-2])
    dxx, dyy, dzz, dxy, dxz, dyz = comps
    return dxx * second_x + dyy * second_y + dzz * second_z + 2.0 * (dxy * cross_xy + dxz * cross_xz + dyz * cross_yz)


def ionic(voltage, gates, calcium):
    fresh = []
    for k in range(6):
        steady = jax.nn.sigmoid(SLOPES[k] * (voltage - MIDDLES[k]))
        fresh.append(steady + (gates[k] - steady) * math.exp(-TIME_STEP * RATES[k]))
    current = (2.0 * fresh[0] * fresh[0] * fresh[0] * fresh[1] * (voltage - 1.2)
               + fresh[2] * fresh[2] * (voltage + 0.1)
               + 0.6 * fresh[3] * fresh[4] * (voltage - 0.9)
               + 0.2 * (1.0 + fresh[5]) * (voltage - 0.05))
    volt_next = voltage - TIME_STEP * current
    calc_next = calcium + TIME_STEP * (1.5 * fresh[3] * fresh[4] * (1.0 - calcium) - 0.8 * calcium)
    return volt_next, fresh, calc_next


def emission(field, tissue_float, which):
    alpha = OPACITY[which] * tissue_float * jax.nn.sigmoid(6.0 * (field - 0.4))
    red = jax.nn.sigmoid(5.0 * (field - 0.5))
    green = jnp.exp(-6.0 * (field - 0.5) * (field - 0.5))
    return alpha, (red, green, 1.0 - red)


def march(alpha, colours):
    through = jnp.cumprod(1.0 - alpha, axis=0)
    before = jnp.concatenate([jnp.ones_like(through[:1]), through[:-1]], axis=0)
    weight = before * alpha
    colour = jnp.stack([jnp.sum(weight * item, axis=0) for item in colours])
    return colour, through[-1]


def advance(voltage, gates, calcium, tissue_float, padded, comps):
    diffused = voltage + TIME_STEP * diffuse(padded, comps)
    volt_next, fresh, calc_next = ionic(diffused, gates, calcium)
    keep = 1.0 - tissue_float
    voltage = tissue_float * volt_next + keep * voltage
    gates = [tissue_float * item + keep * old for item, old in zip(fresh, gates)]
    calcium = tissue_float * calc_next + keep * calcium
    return voltage, gates, calcium


def reference(states, tissue, fiber):
    comps = tensor(fiber)
    tissue_float = expand(tissue).astype(jnp.float32)
    voltage = states[0]
    gates = [states[k] for k in range(1, 7)]
    calcium = states[7]
    images = []
    for step in range(STEPS):
        padded = jnp.pad(voltage * tissue_float, 1)
        voltage, gates, calcium = advance(voltage, gates, calcium, tissue_float, padded, comps)
        pictures = []
        for which, field in enumerate((voltage, calcium)):
            alpha, colours = emission(field, tissue_float, which)
            colour, through = march(alpha, colours)
            pictures.append(jnp.concatenate([colour, (1.0 - through)[None]], axis=0))
        images.append(jnp.stack(pictures))
    final_states = jnp.stack([voltage] + gates + [calcium])
    return final_states, jnp.stack(images)
```

```python
import functools
import math

import jax
import jax.numpy as jnp
from jax import lax
from jax.experimental import pallas as pl
from jax.experimental.pallas import tpu as pltpu
from jax.sharding import PartitionSpec as P

BLK = 4
CLASSES = 8
STEPS = 2
TIME_STEP = 0.15
SIGMA_LONG = 1.0
SIGMA_CROSS = 0.3
SLOPES = (8.0, -8.0, 6.0, 5.0, -5.0, -3.0)
MIDDLES = (0.2, 0.4, 0.3, 0.5, 0.6, 0.5)
RATES = (3.0, 0.5, 1.0, 0.8, 0.3, 0.1)
OPACITY = (0.012, 0.01)
TRACE = 3.0 * SIGMA_CROSS + (SIGMA_LONG - SIGMA_CROSS)
PLANES = 2
MESH = pl.DeviceIdType.MESH


def block_fields(tissue, fiber):
    kind = fiber.astype(jnp.float32)
    polar = math.pi * (kind + 0.5) / CLASSES
    azimuth = 2.3 * kind
    along_x = jnp.cos(polar)
    along_y = jnp.sin(polar) * jnp.cos(azimuth)
    along_z = jnp.sin(polar) * jnp.sin(azimuth)
    spread = SIGMA_LONG - SIGMA_CROSS
    parts = jnp.stack([
        tissue.astype(jnp.float32),
        TIME_STEP * (SIGMA_CROSS + spread * along_x * along_x),
        TIME_STEP * (SIGMA_CROSS + spread * along_y * along_y),
        TIME_STEP * (SIGMA_CROSS + spread * along_z * along_z),
        0.5 * TIME_STEP * spread * along_x * along_y,
        0.5 * TIME_STEP * spread * along_x * along_z,
        0.5 * TIME_STEP * spread * along_y * along_z,
    ])
    fields, first, second, third = parts.shape
    columns = third * BLK
    onehot = (jnp.arange(columns)[None, :] // BLK == jnp.arange(third)[:, None]).astype(jnp.float32)
    rows = jnp.repeat(parts, BLK, axis=2).reshape(fields * first * second * BLK, third)
    wide = jnp.dot(rows, onehot, precision=lax.Precision.HIGHEST, preferred_element_type=jnp.float32)
    return wide.reshape(fields, first, second * BLK, columns)


def halo_kernel(v_ref, mask_ref, hx_ref, hy_ref, xface, yface, xland, yland, send, recv):
    nx, ny = v_ref.shape[1], v_ref.shape[2]
    d, a = lax.axis_index("depth"), lax.axis_index("area")
    nd, na = lax.axis_size("depth"), lax.axis_size("area")
    links = [(i, j) for i in (-1, 0, 1) for j in (-1, 0, 1) if (i, j) != (0, 0)]

    def there(i, j):
        ok = jnp.bool_(True)
        if i:
            ok = jnp.logical_and(ok, d > 0 if i < 0 else d < nd - 1)
        if j:
            ok = jnp.logical_and(ok, a > 0 if j < 0 else a < na - 1)
        return ok

    xland[...] = jnp.zeros_like(xland)
    yland[...] = jnp.zeros_like(yland)
    barrier = pltpu.get_barrier_semaphore()
    for i, j in links:
        @pl.when(there(i, j))
        def _():
            pl.semaphore_signal(barrier, inc=1, device_id=(d + i, a + j), device_id_type=MESH)

    xface[0] = v_ref[0, 0] * mask_ref[0, 0]
    xface[1] = v_ref[0, nx - 1] * mask_ref[0, nx // BLK - 1]
    for x in range(nx):
        yface[0, x:x + 1] = v_ref[0, x, 0:1] * mask_ref[0, x // BLK, 0:1]
        yface[1, x:x + 1] = v_ref[0, x, ny - 1:ny] * mask_ref[0, x // BLK, ny - 1:ny]

    dn = (d > 0).astype(jnp.int32) + (d < nd - 1).astype(jnp.int32)
    an = (a > 0).astype(jnp.int32) + (a < na - 1).astype(jnp.int32)
    pl.semaphore_wait(barrier, dn + an + dn * an)

    def copy(n, i, j):
        if j == 0:
            src, dst = xface.at[0 if i < 0 else 1], xland.at[1 if i < 0 else 0]
        elif i == 0:
            src, dst = yface.at[0 if j < 0 else 1], yland.at[1 if j < 0 else 0, pl.ds(0, nx)]
        else:
            src = yface.at[0 if j < 0 else 1, pl.ds(0 if i < 0 else nx - 1, 1)]
            dst = yland.at[1 if j < 0 else 0, pl.ds(nx + 8 if i < 0 else nx, 1)]
        back = links.index((-i, -j))
        return pltpu.make_async_remote_copy(
            src_ref=src, dst_ref=dst, send_sem=send.at[n], recv_sem=recv.at[back],
            device_id=(d + i, a + j), device_id_type=MESH)

    def arrival(n, i, j):
        back = links.index((-i, -j))
        if j == 0:
            src, dst = xface.at[0 if i > 0 else 1], xland.at[0 if i < 0 else 1]
        elif i == 0:
            src, dst = yface.at[0 if j > 0 else 1], yland.at[0 if j < 0 else 1, pl.ds(0, nx)]
        else:
            src = yface.at[0 if j > 0 else 1, pl.ds(0 if i > 0 else nx - 1, 1)]
            dst = yland.at[0 if j < 0 else 1, pl.ds(nx if i < 0 else nx + 8, 1)]
        return pltpu.make_async_remote_copy(
            src_ref=src, dst_ref=dst, send_sem=send.at[back], recv_sem=recv.at[n],
            device_id=(d + i, a + j), device_id_type=MESH)

    for n, (i, j) in enumerate(links):
        @pl.when(there(i, j))
        def _():
            copy(n, i, j).start()
    for n, (i, j) in enumerate(links):
        @pl.when(there(i, j))
        def _():
            copy(n, i, j).wait_send()
            arrival(n, i, j).wait_recv()
    hx_ref[...] = xland[...]
    hy_ref[...] = yland[...]


def halos(states, mask, collective):
    _, nx, ny, nz = states.shape
    whole = pl.BlockSpec(memory_space=pltpu.VMEM)
    return pl.pallas_call(
        halo_kernel,
        grid=(1,),
        out_shape=(jax.ShapeDtypeStruct((2, ny, nz), jnp.float32),
                   jax.ShapeDtypeStruct((2, nx + 16, nz), jnp.float32)),
        in_specs=[pl.BlockSpec((1, nx, ny, nz), lambda i: (0, 0, 0, 0)),
                  pl.BlockSpec((1,) + mask.shape[1:], lambda i: (0, 0, 0, 0))],
        out_specs=(whole, whole),
        scratch_shapes=[
            pltpu.VMEM((2, ny, nz), jnp.float32),
            pltpu.VMEM((2, nx, nz), jnp.float32),
            pltpu.VMEM((2, ny, nz), jnp.float32),
            pltpu.VMEM((2, nx + 16, nz), jnp.float32),
            pltpu.SemaphoreType.DMA((8,)),
            pltpu.SemaphoreType.DMA((8,)),
        ],
        compiler_params=pltpu.CompilerParams(
            collective_id=collective, has_side_effects=True, vmem_limit_bytes=16 << 20),
        name="halo%d" % collective,
    )(states, mask)


def step_kernel(in_ref, v_ref, field_ref, hx_ref, hy_ref, out_ref, acc_ref, pad):
    nx, ny, nz = v_ref.shape[1:]
    i = pl.program_id(0)

    @pl.when(i == 0)
    def _():
        pad[:, :, nz:] = jnp.zeros((nx + 2, ny + 16, pad.shape[2] - nz), jnp.float32)
        acc_ref[...] = jnp.zeros_like(acc_ref)
        for x in range(nx):
            pad[x + 1, 8:8 + ny, :nz] = v_ref[0, x] * field_ref[0, x // BLK]
        pad[0, 8:8 + ny, :nz] = hx_ref[0]
        pad[nx + 1, 8:8 + ny, :nz] = hx_ref[1]
        for side, row in ((0, 7), (1, 8 + ny)):
            pad[0, row:row + 1, :nz] = hy_ref[side, nx:nx + 1]
            pad[nx + 1, row:row + 1, :nz] = hy_ref[side, nx + 8:nx + 9]
            for x in range(nx):
                pad[x + 1, row:row + 1, :nz] = hy_ref[side, x:x + 1]

    wide = pad.shape[2]

    def plane(p):
        x = i * PLANES + p
        block = x // BLK
        for top in range(0, ny, 8):
            def rows(dx, dy):
                return pad[x + 1 + dx, 8 + top + dy:16 + top + dy, :]

            centre = rows(0, 0)
            up, down = rows(0, -1), rows(0, 1)
            after, before = rows(1, 0), rows(-1, 0)
            slope_x = after - before
            slope_y = down - up
            slope_xy = (rows(1, 1) - rows(-1, 1)) - (rows(1, -1) - rows(-1, -1))

            def ahead(item):
                return pltpu.roll(item, wide - 1, 1)

            def behind(item):
                return pltpu.roll(item, 1, 1)

            second_z = ahead(centre) + behind(centre)
            slope_xz = ahead(slope_x) - behind(slope_x)
            slope_yz = ahead(slope_y) - behind(slope_y)
            second_x = after + before
            second_y = up + down
            for left in range(0, nz, 128):
                zs = slice(left, left + 128)
                at = (slice(top, top + 8), zs)

                def comp(k):
                    return field_ref[k, block, top:top + 8, zs]

                w = ((1.0 - 2.0 * TIME_STEP * TRACE) * centre[:, zs]
                     + comp(1) * second_x[:, zs] + comp(2) * second_y[:, zs] + comp(3) * second_z[:, zs]
                     + comp(4) * slope_xy[:, zs] + comp(5) * slope_xz[:, zs] + comp(6) * slope_yz[:, zs])
                mask = comp(0)
                tissue = mask > 0.5
                h = []
                for k in range(6):
                    decay = math.exp(-TIME_STEP * RATES[k])
                    half = 0.5 * (1.0 - decay)
                    old = in_ref[k + 1, p, top:top + 8, zs]
                    gate = old * decay + (half + half * jnp.tanh(
                        (0.5 * SLOPES[k]) * w - 0.5 * SLOPES[k] * MIDDLES[k]))
                    h.append(gate)
                    out_ref[k + 1, p, top:top + 8, zs] = jnp.where(tissue, gate, old)
                pair = h[3] * h[4]
                current = (
                    (h[0] * h[0]) * (h[0] * h[1]) * (2.0 * w - 2.4)
                    + h[2] * h[2] * (w + 0.1)
                    + pair * (0.6 * w - 0.54)
                    + (1.0 + h[5]) * (0.2 * w - 0.01)
                )
                old_v = in_ref[0, p, top:top + 8, zs]
                old_ca = in_ref[7, p, top:top + 8, zs]
                volt = jnp.where(tissue, w - TIME_STEP * current, old_v)
                calc = jnp.where(
                    tissue,
                    (1.0 - 0.8 * TIME_STEP) * old_ca + (1.5 * TIME_STEP) * pair * (1.0 - old_ca),
                    old_ca)
                out_ref[0, p, top:top + 8, zs] = volt
                out_ref[7, p, top:top + 8, zs] = calc
                for which, q in enumerate((volt, calc)):
                    half = (0.5 * OPACITY[which]) * mask
                    alpha = half + half * jnp.tanh(3.0 * q - 1.2)
                    total = acc_ref[(3 * which,) + at]
                    weight = (1.0 - total) * alpha
                    acc_ref[(3 * which,) + at] = total + weight
                    acc_ref[(3 * which + 1,) + at] += weight * jnp.tanh(2.5 * q - 1.25)
                    off = q - 0.5
                    acc_ref[(3 * which + 2,) + at] += weight * jnp.exp(-6.0 * off * off)

    for p in range(PLANES):
        plane(p)


def advance(states, fields, hx, hy):
    _, nx, ny, nz = states.shape
    whole = pl.BlockSpec(memory_space=pltpu.VMEM)
    return pl.pallas_call(
        step_kernel,
        grid=(nx // PLANES,),
        out_shape=(jax.ShapeDtypeStruct(states.shape, jnp.float32),
                   jax.ShapeDtypeStruct((6, ny, nz), jnp.float32)),
        in_specs=[pl.BlockSpec((8, PLANES, ny, nz), lambda i: (0, i, 0, 0)),
                  pl.BlockSpec((1, nx, ny, nz), lambda i: (0, 0, 0, 0)),
                  whole, whole, whole],
        out_specs=(pl.BlockSpec((8, PLANES, ny, nz), lambda i: (0, i, 0, 0)),
                   pl.BlockSpec((6, ny, nz), lambda i: (0, 0, 0))),
        scratch_shapes=[pltpu.VMEM((nx + 2, ny + 16, nz + 128), jnp.float32)],
        compiler_params=pltpu.CompilerParams(vmem_limit_bytes=32 << 20),
        name="step",
    )(states, states, fields, hx, hy)


def blend_kernel(part_ref, out_ref, land, send, recv):
    count = part_ref.shape[0]
    me = lax.axis_index("depth")
    barrier = pltpu.get_barrier_semaphore()
    for k in range(1, count):
        pl.semaphore_signal(barrier, inc=1, device_id={"depth": lax.rem(me + k, count)}, device_id_type=MESH)
    pl.semaphore_wait(barrier, count - 1)
    copies = []
    for k in range(1, count):
        to = lax.rem(me + k, count)
        copy = pltpu.make_async_remote_copy(
            src_ref=part_ref.at[to], dst_ref=land.at[k], send_sem=send.at[k], recv_sem=recv.at[k],
            device_id={"depth": to}, device_id_type=MESH)
        copy.start()
        copies.append(copy)
    land[0] = part_ref[me]
    for copy in copies:
        copy.wait()
    images, ny = out_ref.shape[0], out_ref.shape[2]
    for n in range(images):
        def at(group, channel):
            start = (3 * n + channel) * ny
            return land[lax.rem(me - group + count, count), start:start + ny]

        total, warm, green = at(0, 0), at(0, 1), at(0, 2)
        for group in range(1, count):
            through = 1.0 - total
            warm = warm + through * at(group, 1)
            green = green + through * at(group, 2)
            total = total + through * at(group, 0)
        out_ref[n, 0] = 0.5 * (total + warm)
        out_ref[n, 1] = green
        out_ref[n, 2] = 0.5 * (total - warm)
        out_ref[n, 3] = total


def blend(parts):
    steps, _, ny, nz = parts.shape
    count = lax.axis_size("depth")
    width = nz // count
    split = jnp.moveaxis(parts.reshape(steps * 6 * ny, count, width), 1, 0)
    out = pl.pallas_call(
        blend_kernel,
        out_shape=jax.ShapeDtypeStruct((steps * 2, 4, ny, width), jnp.float32),
        in_specs=[pl.BlockSpec(memory_space=pltpu.VMEM)],
        out_specs=pl.BlockSpec(memory_space=pltpu.VMEM),
        scratch_shapes=[
            pltpu.VMEM((count, steps * 6 * ny, width), jnp.float32),
            pltpu.SemaphoreType.DMA((count,)),
            pltpu.SemaphoreType.DMA((count,)),
        ],
        compiler_params=pltpu.CompilerParams(
            collective_id=7, has_side_effects=True, vmem_limit_bytes=16 << 20),
        name="blend",
    )(split)
    return out.reshape(steps, 2, 4, ny, width)


def per_device(states, tissue, fiber):
    fields = block_fields(tissue, fiber)
    parts = []
    for step in range(STEPS):
        hx, hy = halos(states, fields, step)
        states, part = advance(states, fields, hx, hy)
        parts.append(part)
    return states, blend(jnp.stack(parts))


def solution(mesh):
    return jax.shard_map(
        per_device,
        mesh=mesh,
        in_specs=(
            P(None, "depth", "area", None),
            P("depth", "area", None),
            P("depth", "area", None),
        ),
        out_specs=(P(None, "depth", "area", None), P(None, None, None, "area", "depth")),
        check_vma=False,
    )
```

```python
import functools
import math

import jax
import jax.numpy as jnp
from jax import lax
from jax.experimental import pallas as pl
from jax.experimental.pallas import tpu as pltpu
from jax.sharding import PartitionSpec as P

BLK = 4
CLASSES = 8
STEPS = 2
TIME_STEP = 0.15
SIGMA_LONG = 1.0
SIGMA_CROSS = 0.3
SLOPES = (8.0, -8.0, 6.0, 5.0, -5.0, -3.0)
MIDDLES = (0.2, 0.4, 0.3, 0.5, 0.6, 0.5)
RATES = (3.0, 0.5, 1.0, 0.8, 0.3, 0.1)
OPACITY = (0.012, 0.01)
TRACE = 3.0 * SIGMA_CROSS + (SIGMA_LONG - SIGMA_CROSS)
PLANES = 2
MESH = pl.DeviceIdType.MESH


def components(kind):
    polar = math.pi * (kind + 0.5) / CLASSES
    azimuth = 2.3 * kind
    fx = math.cos(polar)
    fy = math.sin(polar) * math.cos(azimuth)
    fz = math.sin(polar) * math.sin(azimuth)
    spread = SIGMA_LONG - SIGMA_CROSS
    return (
        TIME_STEP * (SIGMA_CROSS + spread * fx * fx),
        TIME_STEP * (SIGMA_CROSS + spread * fy * fy),
        TIME_STEP * (SIGMA_CROSS + spread * fz * fz),
        0.5 * TIME_STEP * spread * fx * fy,
        0.5 * TIME_STEP * spread * fx * fz,
        0.5 * TIME_STEP * spread * fy * fz,
    )


def fields_kernel(tissue_ref, fiber_ref, out_ref):
    first, second, third = tissue_ref.shape
    columns = third * BLK
    table = [components(c) for c in range(CLASSES)]
    onehot = (lax.broadcasted_iota(jnp.int32, (third, columns), 1) // BLK
              == lax.broadcasted_iota(jnp.int32, (third, columns), 0)).astype(jnp.float32)
    for x in range(first):
        kind = fiber_ref[x]
        parts = [tissue_ref[x].astype(jnp.float32)]
        for k in range(6):
            value = jnp.full(kind.shape, table[0][k], jnp.float32)
            for c in range(1, CLASSES):
                value = jnp.where(kind == c, table[c][k], value)
            parts.append(value)
        rows = jnp.concatenate(parts, axis=0)
        wide = jnp.dot(rows, onehot, precision=lax.Precision.HIGHEST, preferred_element_type=jnp.float32)
        for k in range(7):
            for y in range(second):
                row = k * second + y
                out_ref[k, x, y * BLK:(y + 1) * BLK, :] = jnp.broadcast_to(wide[row:row + 1], (BLK, columns))


def block_fields(tissue, fiber):
    first, second, third = tissue.shape
    whole = pl.BlockSpec(memory_space=pltpu.VMEM)
    return pl.pallas_call(
        fields_kernel,
        out_shape=jax.ShapeDtypeStruct((7, first, second * BLK, third * BLK), jnp.float32),
        in_specs=[whole, whole],
        out_specs=whole,
        compiler_params=pltpu.CompilerParams(vmem_limit_bytes=16 << 20),
        name="fields",
    )(tissue, fiber)


def halo_kernel(v_ref, mask_ref, hx_ref, hy_ref, xface, yface, xland, yland, send, recv):
    nx, ny = v_ref.shape[1], v_ref.shape[2]
    d, a = lax.axis_index("depth"), lax.axis_index("area")
    nd, na = lax.axis_size("depth"), lax.axis_size("area")
    links = [(i, j) for i in (-1, 0, 1) for j in (-1, 0, 1) if (i, j) != (0, 0)]

    def there(i, j):
        ok = jnp.bool_(True)
        if i:
            ok = jnp.logical_and(ok, d > 0 if i < 0 else d < nd - 1)
        if j:
            ok = jnp.logical_and(ok, a > 0 if j < 0 else a < na - 1)
        return ok

    xland[...] = jnp.zeros_like(xland)
    yland[...] = jnp.zeros_like(yland)
    barrier = pltpu.get_barrier_semaphore()
    for i, j in links:
        @pl.when(there(i, j))
        def _():
            pl.semaphore_signal(barrier, inc=1, device_id=(d + i, a + j), device_id_type=MESH)

    xface[0] = v_ref[0, 0] * mask_ref[0, 0]
    xface[1] = v_ref[0, nx - 1] * mask_ref[0, nx // BLK - 1]
    for x in range(nx):
        yface[0, x:x + 1] = v_ref[0, x, 0:1] * mask_ref[0, x // BLK, 0:1]
        yface[1, x:x + 1] = v_ref[0, x, ny - 1:ny] * mask_ref[0, x // BLK, ny - 1:ny]

    dn = (d > 0).astype(jnp.int32) + (d < nd - 1).astype(jnp.int32)
    an = (a > 0).astype(jnp.int32) + (a < na - 1).astype(jnp.int32)
    pl.semaphore_wait(barrier, dn + an + dn * an)

    def copy(n, i, j):
        if j == 0:
            src, dst = xface.at[0 if i < 0 else 1], xland.at[1 if i < 0 else 0]
        elif i == 0:
            src, dst = yface.at[0 if j < 0 else 1], yland.at[1 if j < 0 else 0, pl.ds(0, nx)]
        else:
            src = yface.at[0 if j < 0 else 1, pl.ds(0 if i < 0 else nx - 1, 1)]
            dst = yland.at[1 if j < 0 else 0, pl.ds(nx + 8 if i < 0 else nx, 1)]
        back = links.index((-i, -j))
        return pltpu.make_async_remote_copy(
            src_ref=src, dst_ref=dst, send_sem=send.at[n], recv_sem=recv.at[back],
            device_id=(d + i, a + j), device_id_type=MESH)

    def arrival(n, i, j):
        back = links.index((-i, -j))
        if j == 0:
            src, dst = xface.at[0 if i > 0 else 1], xland.at[0 if i < 0 else 1]
        elif i == 0:
            src, dst = yface.at[0 if j > 0 else 1], yland.at[0 if j < 0 else 1, pl.ds(0, nx)]
        else:
            src = yface.at[0 if j > 0 else 1, pl.ds(0 if i > 0 else nx - 1, 1)]
            dst = yland.at[0 if j < 0 else 1, pl.ds(nx if i < 0 else nx + 8, 1)]
        return pltpu.make_async_remote_copy(
            src_ref=src, dst_ref=dst, send_sem=send.at[back], recv_sem=recv.at[n],
            device_id=(d + i, a + j), device_id_type=MESH)

    for n, (i, j) in enumerate(links):
        @pl.when(there(i, j))
        def _():
            copy(n, i, j).start()
    for n, (i, j) in enumerate(links):
        @pl.when(there(i, j))
        def _():
            copy(n, i, j).wait_send()
            arrival(n, i, j).wait_recv()
    hx_ref[...] = xland[...]
    hy_ref[...] = yland[...]


def halos(states, mask, collective):
    _, nx, ny, nz = states.shape
    whole = pl.BlockSpec(memory_space=pltpu.VMEM)
    return pl.pallas_call(
        halo_kernel,
        grid=(1,),
        out_shape=(jax.ShapeDtypeStruct((2, ny, nz), jnp.float32),
                   jax.ShapeDtypeStruct((2, nx + 16, nz), jnp.float32)),
        in_specs=[pl.BlockSpec((1, nx, ny, nz), lambda i: (0, 0, 0, 0)),
                  pl.BlockSpec((1,) + mask.shape[1:], lambda i: (0, 0, 0, 0))],
        out_specs=(whole, whole),
        scratch_shapes=[
            pltpu.VMEM((2, ny, nz), jnp.float32),
            pltpu.VMEM((2, nx, nz), jnp.float32),
            pltpu.VMEM((2, ny, nz), jnp.float32),
            pltpu.VMEM((2, nx + 16, nz), jnp.float32),
            pltpu.SemaphoreType.DMA((8,)),
            pltpu.SemaphoreType.DMA((8,)),
        ],
        compiler_params=pltpu.CompilerParams(
            collective_id=collective, has_side_effects=True, vmem_limit_bytes=16 << 20),
        name="halo%d" % collective,
    )(states, mask)


def step_kernel(in_ref, v_ref, field_ref, hx_ref, hy_ref, out_ref, acc_ref, pad):
    nx, ny, nz = v_ref.shape[1:]
    i = pl.program_id(0)

    @pl.when(i == 0)
    def _():
        pad[:, :, nz:] = jnp.zeros((nx + 2, ny + 16, pad.shape[2] - nz), jnp.float32)
        acc_ref[...] = jnp.zeros_like(acc_ref)
        for x in range(nx):
            pad[x + 1, 8:8 + ny, :nz] = v_ref[0, x] * field_ref[0, x // BLK]
        pad[0, 8:8 + ny, :nz] = hx_ref[0]
        pad[nx + 1, 8:8 + ny, :nz] = hx_ref[1]
        for side, row in ((0, 7), (1, 8 + ny)):
            pad[0, row:row + 1, :nz] = hy_ref[side, nx:nx + 1]
            pad[nx + 1, row:row + 1, :nz] = hy_ref[side, nx + 8:nx + 9]
            for x in range(nx):
                pad[x + 1, row:row + 1, :nz] = hy_ref[side, x:x + 1]

    wide = pad.shape[2]

    def plane(p):
        x = i * PLANES + p
        block = x // BLK
        for top in range(0, ny, 8):
            def rows(dx, dy):
                return pad[x + 1 + dx, 8 + top + dy:16 + top + dy, :]

            centre = rows(0, 0)
            up, down = rows(0, -1), rows(0, 1)
            after, before = rows(1, 0), rows(-1, 0)
            slope_x = after - before
            slope_y = down - up
            slope_xy = (rows(1, 1) - rows(-1, 1)) - (rows(1, -1) - rows(-1, -1))

            def ahead(item):
                return pltpu.roll(item, wide - 1, 1)

            def behind(item):
                return pltpu.roll(item, 1, 1)

            second_z = ahead(centre) + behind(centre)
            slope_xz = ahead(slope_x) - behind(slope_x)
            slope_yz = ahead(slope_y) - behind(slope_y)
            second_x = after + before
            second_y = up + down
            for left in range(0, nz, 128):
                zs = slice(left, left + 128)
                at = (slice(top, top + 8), zs)

                def comp(k):
                    return field_ref[k, block, top:top + 8, zs]

                w = ((1.0 - 2.0 * TIME_STEP * TRACE) * centre[:, zs]
                     + comp(1) * second_x[:, zs] + comp(2) * second_y[:, zs] + comp(3) * second_z[:, zs]
                     + comp(4) * slope_xy[:, zs] + comp(5) * slope_xz[:, zs] + comp(6) * slope_yz[:, zs])
                mask = comp(0)
                tissue = mask > 0.5
                h = []
                for k in range(6):
                    decay = math.exp(-TIME_STEP * RATES[k])
                    half = 0.5 * (1.0 - decay)
                    old = in_ref[k + 1, p, top:top + 8, zs]
                    gate = old * decay + (half + half * jnp.tanh(
                        (0.5 * SLOPES[k]) * w - 0.5 * SLOPES[k] * MIDDLES[k]))
                    h.append(gate)
                    out_ref[k + 1, p, top:top + 8, zs] = jnp.where(tissue, gate, old)
                pair = h[3] * h[4]
                current = (
                    (h[0] * h[0]) * (h[0] * h[1]) * (2.0 * w - 2.4)
                    + h[2] * h[2] * (w + 0.1)
                    + pair * (0.6 * w - 0.54)
                    + (1.0 + h[5]) * (0.2 * w - 0.01)
                )
                old_v = in_ref[0, p, top:top + 8, zs]
                old_ca = in_ref[7, p, top:top + 8, zs]
                volt = jnp.where(tissue, w - TIME_STEP * current, old_v)
                calc = jnp.where(
                    tissue,
                    (1.0 - 0.8 * TIME_STEP) * old_ca + (1.5 * TIME_STEP) * pair * (1.0 - old_ca),
                    old_ca)
                out_ref[0, p, top:top + 8, zs] = volt
                out_ref[7, p, top:top + 8, zs] = calc
                for which, q in enumerate((volt, calc)):
                    half = (0.5 * OPACITY[which]) * mask
                    alpha = half + half * jnp.tanh(3.0 * q - 1.2)
                    total = acc_ref[(3 * which,) + at]
                    weight = (1.0 - total) * alpha
                    acc_ref[(3 * which,) + at] = total + weight
                    acc_ref[(3 * which + 1,) + at] += weight * jnp.tanh(2.5 * q - 1.25)
                    off = q - 0.5
                    acc_ref[(3 * which + 2,) + at] += weight * jnp.exp(-6.0 * off * off)

    for p in range(PLANES):
        plane(p)


def advance(states, fields, hx, hy):
    _, nx, ny, nz = states.shape
    whole = pl.BlockSpec(memory_space=pltpu.VMEM)
    return pl.pallas_call(
        step_kernel,
        grid=(nx // PLANES,),
        out_shape=(jax.ShapeDtypeStruct(states.shape, jnp.float32),
                   jax.ShapeDtypeStruct((6, ny, nz), jnp.float32)),
        in_specs=[pl.BlockSpec((8, PLANES, ny, nz), lambda i: (0, i, 0, 0)),
                  pl.BlockSpec((1, nx, ny, nz), lambda i: (0, 0, 0, 0)),
                  whole, whole, whole],
        out_specs=(pl.BlockSpec((8, PLANES, ny, nz), lambda i: (0, i, 0, 0)),
                   pl.BlockSpec((6, ny, nz), lambda i: (0, 0, 0))),
        scratch_shapes=[pltpu.VMEM((nx + 2, ny + 16, nz + 128), jnp.float32)],
        compiler_params=pltpu.CompilerParams(vmem_limit_bytes=32 << 20),
        name="step",
    )(states, states, fields, hx, hy)


def blend_kernel(base, rem, *refs):
    kinds = (base > 0) + (rem > 0)
    parts, out_ref, lands = refs[:kinds], refs[kinds], refs[kinds + 1:2 * kinds + 1]
    send, recv = refs[2 * kinds + 1:]
    count = parts[0].shape[0]
    me = lax.axis_index("depth")
    barrier = pltpu.get_barrier_semaphore()
    for k in range(1, count):
        pl.semaphore_signal(barrier, inc=1, device_id={"depth": lax.rem(me + k, count)}, device_id_type=MESH)
    pl.semaphore_wait(barrier, count - 1)
    copies = []
    for k in range(1, count):
        to = lax.rem(me + k, count)
        for n in range(kinds):
            copy = pltpu.make_async_remote_copy(
                src_ref=parts[n].at[to], dst_ref=lands[n].at[k], send_sem=send.at[n, k],
                recv_sem=recv.at[n, k], device_id={"depth": to}, device_id_type=MESH)
            copy.start()
            copies.append(copy)
    for n in range(kinds):
        lands[n][0] = parts[n][me]
    for copy in copies:
        copy.wait()
    images, ny = out_ref.shape[0], out_ref.shape[2]
    pieces = [(0, 0, base)] if base else []
    if rem:
        pieces.append((kinds - 1, base, rem))
    for which, left, width in pieces:
        height = lands[which].shape[1]
        for n in range(images):
            def at(group, channel):
                start = (3 * n + channel) * ny
                lane = (start // height) * width
                start = start % height
                return lands[which][lax.rem(me - group + count, count), start:start + ny, lane:lane + width]

            total, warm, green = at(0, 0), at(0, 1), at(0, 2)
            for group in range(1, count):
                through = 1.0 - total
                warm = warm + through * at(group, 1)
                green = green + through * at(group, 2)
                total = total + through * at(group, 0)
            zs = slice(left, left + width)
            out_ref[n, 0, :, zs] = 0.5 * (total + warm)
            out_ref[n, 1, :, zs] = green
            out_ref[n, 2, :, zs] = 0.5 * (total - warm)
            out_ref[n, 3, :, zs] = total


def blend(parts):
    steps, _, ny, nz = parts.shape
    count = lax.axis_size("depth")
    width = nz // count
    rem = width % 128
    base = width - rem
    rows = steps * 6 * ny
    split = jnp.moveaxis(parts.reshape(rows, count, width), 1, 0)
    sent = [split[:, :, :base]] if base else []
    if rem:
        fold = 128 // rem
        while (steps * 6) % fold:
            fold -= 1
        tall = rows // fold
        sent.append(jnp.concatenate(
            [split[:, f * tall:(f + 1) * tall, base:] for f in range(fold)], axis=2))
    out = pl.pallas_call(
        functools.partial(blend_kernel, base, rem),
        out_shape=jax.ShapeDtypeStruct((steps * 2, 4, ny, width), jnp.float32),
        in_specs=[pl.BlockSpec(memory_space=pltpu.VMEM)] * len(sent),
        out_specs=pl.BlockSpec(memory_space=pltpu.VMEM),
        scratch_shapes=[pltpu.VMEM(item.shape, jnp.float32) for item in sent] + [
            pltpu.SemaphoreType.DMA((len(sent), count)),
            pltpu.SemaphoreType.DMA((len(sent), count)),
        ],
        compiler_params=pltpu.CompilerParams(
            collective_id=7, has_side_effects=True, vmem_limit_bytes=16 << 20),
        name="blend",
    )(*sent)
    return out.reshape(steps, 2, 4, ny, width)


def per_device(states, tissue, fiber):
    fields = block_fields(tissue, fiber)
    parts = []
    for step in range(STEPS):
        hx, hy = halos(states if step else states[:1], fields, step)
        states, part = advance(states, fields, hx, hy)
        parts.append(part)
    return states, blend(jnp.stack(parts))


def solution(mesh):
    return jax.shard_map(
        per_device,
        mesh=mesh,
        in_specs=(
            P(None, "depth", "area", None),
            P("depth", "area", None),
            P("depth", "area", None),
        ),
        out_specs=(P(None, "depth", "area", None), P(None, None, None, "area", "depth")),
        check_vma=False,
    )
```
